32 devices in a mesh: seq: 4 (over z), head: 4 (over y, x), batch: 2 (over core).
Axes of the slice: x: 2, y: 2, z: 4, core: 2. Of those that a mesh axis runs over, the one named last changes fastest.
Arguments:
- tokens: bfloat16 [4096, 2560], P(('batch', 'seq'), 'head'), parts along dimension 0, may hold values from -6 to 6
- resets: int32 [4096], P(('batch', 'seq')), parts along dimension 0, may hold values 0 or 1
- w_x: bfloat16 [2560, 5120], P(None, 'head'), may hold values from -0.125 to 0.125
- w_z: bfloat16 [2560, 5120], P(None, 'head'), may hold values from -0.125 to 0.125
- w_bc: bfloat16 [2560, 256], replicated, may hold values from -0.125 to 0.125
- w_dt: bfloat16 [2560, 80], P(None, 'head'), may hold values from -0.125 to 0.125
- dt_bias: float32 [80], P('head'), may hold values from -2 to 1
- decay_rate: float32 [80], P('head'), may hold values from 0.00024414062 to 0.08
- d_skip: float32 [80], P('head'), may hold values from 0.5 to 1.5
- norm_gain: float32 [5120], P('head'), may hold values from 0.5 to 1.5
- w_out: bfloat16 [5120, 2560], P('head'), may hold values from -0.078125 to 0.078125
Outputs:
- mixed: bfloat16 [4096, 2560], P(('batch', 'seq'), 'head'), parts along dimension 0
The draws below stay inside these ranges and needn't reach their ends.
There are 2 independent parts, one for each index of `batch`. The reference program is written for one: setup_inputs(seed, part) draws one part's arguments, and reference() takes and returns one part's arrays. A program takes and returns all parts, laid end to end along the dimension named above; an argument that names none is the same for every part. Nothing has to cross between parts.
All inputs are finite; a program needn't handle non-finite values. No bound on the sum of `resets` on one device may be relied on, other than what follows from the above.
Results may differ from the reference program's by a relative error of at most 0.013.
Values may be sent and summed in bfloat16 or wider, within the bound.
A program may use at most 128 MiB of HBM per device.

```python
import math
import jax
import jax.numpy as jnp
from jax import lax

D = 2560
DI = 5120
HEADS = 80
HEADDIM = 64
NSTATE = 128
L_DEV = 512
GROUP = 256
LENGTH = 2048


def with_ends(array, own_key, smallest, high):
    longest = array.shape.index(max(array.shape))
    spots = []
    for shift in (0, 1):
        where = [jax.random.randint(jax.random.fold_in(own_key, axis), (), 0, length) for axis, length in enumerate(array.shape)]
        where[longest] = (where[longest] + shift) % array.shape[longest]
        spots.append(tuple(where))
    return array.at[spots[0]].set(smallest).at[spots[1]].set(high)


def level_of(stream_key, extent, cuts, least, high):
    level, own = 1.0, jax.random.fold_in(stream_key, 6)
    for dim, shards_of in cuts:
        heights = jnp.exp(jax.random.uniform(jax.random.fold_in(own, dim), (shards_of,), jnp.float32, least / len(cuts), high / len(cuts)))
        level = level * jnp.repeat(heights, extent[dim] // shards_of).reshape([-1 if axis == dim else 1 for axis in range(len(extent))])
    return level


def normal_values(own_key, dims, scale, most, split=(), kind=jnp.bfloat16):
    result = scale * jax.random.normal(own_key, dims, jnp.float32)
    if split:
        result = result * level_of(own_key, dims, split, -0.22, 0.18)
    return jnp.clip(result, -most, most).astype(kind)


def setup_inputs(seed: int = 0, part: int = 0) -> dict:
    keys = jax.random.split(jax.random.key(seed), 12)
    part_splits = jax.random.split(jax.random.fold_in(keys[11], part), 12)
    tokens = normal_values(part_splits[0], (LENGTH, D), 1.0, 6.0, ((0, 4), (1, 4)))
    resets = with_ends((jax.random.randint(part_splits[1], (LENGTH,), 0, 2 * L_DEV) < 1).astype(jnp.int32), jax.random.fold_in(part_splits[1], 1), 0, 1)
    w_x = normal_values(keys[2], (D, DI), D ** -0.5, 0.125, ((1, 4),))
    w_z = normal_values(keys[3], (D, DI), D ** -0.5, 0.125, ((1, 4),))
    w_bc = normal_values(keys[4], (D, 2 * NSTATE), D ** -0.5, 0.125)
    w_dt = normal_values(keys[5], (D, HEADS), D ** -0.5, 0.125, ((1, 4),))
    dt_bias = jnp.clip(-2.0 + 3.0 * jax.random.uniform(keys[6], (HEADS,), jnp.float32) ** level_of(keys[6], (HEADS,), ((0, 4),), -0.2, 0.2), -2.0, 1.0)
    decay_rate = jnp.clip(jnp.exp(math.log(0.08) - 5.7920375 * jax.random.uniform(keys[7], (HEADS,), jnp.float32) ** level_of(keys[7], (HEADS,), ((0, 4),), -0.2, 0.2)), 0.00024414062, 0.08)
    d_skip = jnp.clip(0.5 + 1.0 * jax.random.uniform(keys[8], (HEADS,), jnp.float32) ** level_of(keys[8], (HEADS,), ((0, 4),), -0.2, 0.2), 0.5, 1.5)
    norm_gain = jnp.clip(1.0 + 0.1 * jax.random.normal(keys[9], (DI,), jnp.float32), 0.5, 1.5)
    w_out = normal_values(keys[10], (DI, D), DI ** -0.5, 0.078125, ((0, 4),))
    return {"tokens": tokens, "resets": resets, "w_x": w_x, "w_z": w_z, "w_bc": w_bc, "w_dt": w_dt, "dt_bias": dt_bias, "decay_rate": decay_rate, "d_skip": d_skip, "norm_gain": norm_gain, "w_out": w_out}


def decay_block(inputs, step_size, log_decay, in_proj, out_proj, restart, state_in):
    cumulative = jnp.cumsum(log_decay, axis=0)
    segment = jnp.cumsum(restart)
    places = jnp.arange(restart.shape[0], dtype=jnp.int32)
    same_doc = (segment[:, None] == segment[None, :]) & (places[:, None] >= places[None, :])
    scores = jnp.dot(out_proj, in_proj.T, preferred_element_type=jnp.float32)
    spread = cumulative.T[:, :, None] - cumulative.T[:, None, :]
    factor = jnp.exp(jnp.where(same_doc[None], spread, -jnp.inf))
    mixing = (factor * scores[None] * step_size.T[:, None, :]).astype(jnp.bfloat16)
    output = jnp.einsum('hts,shp->thp', mixing.astype(jnp.float32), inputs.astype(jnp.float32))
    entering = jnp.where((segment == 0)[:, None], jnp.exp(cumulative), 0.0)
    carried = jnp.einsum('tn,hpn->thp', out_proj.astype(jnp.float32), state_in, precision=lax.Precision.HIGHEST)
    output = output + entering[:, :, None] * carried
    closing = segment[-1]
    keeping = jnp.where((segment == closing)[:, None], jnp.exp(cumulative[-1][None, :] - cumulative), 0.0) * step_size
    scaled = (keeping[:, :, None] * inputs.astype(jnp.float32)).astype(jnp.bfloat16)
    update = jnp.einsum('shp,sn->hpn', scaled.astype(jnp.float32), in_proj.astype(jnp.float32))
    through = jnp.where(closing == 0, jnp.exp(cumulative[-1]), 0.0)
    return (output, update + through[:, None, None] * state_in)

def reference(tokens, resets, w_x, w_z, w_bc, w_dt, dt_bias, decay_rate, d_skip, norm_gain, w_out):
    inner = jax.nn.silu(jnp.dot(tokens, w_x, preferred_element_type=jnp.float32)).astype(jnp.bfloat16)
    gating = jnp.dot(tokens, w_z, preferred_element_type=jnp.float32).astype(jnp.bfloat16)
    mapped = jax.nn.silu(jnp.dot(tokens, w_bc, preferred_element_type=jnp.float32)).astype(jnp.bfloat16)
    step_size = jax.nn.softplus(jnp.dot(tokens, w_dt, preferred_element_type=jnp.float32) + dt_bias)
    log_decay = -step_size * decay_rate
    blocks = LENGTH // GROUP
    sliced = (inner.reshape(blocks, GROUP, HEADS, HEADDIM), step_size.reshape(blocks, GROUP, HEADS), log_decay.reshape(blocks, GROUP, HEADS), mapped[:, :NSTATE].reshape(blocks, GROUP, NSTATE), mapped[:, NSTATE:].reshape(blocks, GROUP, NSTATE), resets.reshape(blocks, GROUP))

    def advance(state_in, pieces):
        output, state_out = decay_block(pieces[0], pieces[1], pieces[2], pieces[3], pieces[4], pieces[5], state_in)
        return (state_out, output)
    final_state, outputs = lax.scan(advance, jnp.zeros((HEADS, HEADDIM, NSTATE), jnp.float32), sliced)
    mixed_heads = outputs.reshape(LENGTH, HEADS, HEADDIM) + d_skip[None, :, None] * inner.reshape(LENGTH, HEADS, HEADDIM).astype(jnp.float32)
    gated = mixed_heads.reshape(LENGTH, DI) * jax.nn.silu(gating.astype(jnp.float32))
    meansq = lax.optimization_barrier(jnp.mean(gated * gated, axis=1, keepdims=True))
    normed = (gated * lax.rsqrt(meansq + 1e-05) * norm_gain).astype(jnp.bfloat16)
    return jnp.dot(normed, w_out, preferred_element_type=jnp.float32).astype(jnp.bfloat16)
```

```python
import functools

import jax
import jax.numpy as jnp
from jax import lax
from jax.experimental import pallas as pl
from jax.experimental.pallas import tpu as pltpu
from jax.sharding import PartitionSpec as P

HEADDIM = 64
NSTATE = 128
GROUP = 256
LANES = 128
F32 = jnp.float32
BF16 = jnp.bfloat16
MESH = pl.DeviceIdType.MESH
VMEM = pl.BlockSpec(memory_space=pltpu.VMEM)
SMEM = pl.BlockSpec(memory_space=pltpu.SMEM)
ANY = pl.BlockSpec(memory_space=pl.ANY)
EPS = 1e-05


def peers():
    me = lax.axis_index("head")
    across = me + 1 - 2 * lax.rem(me, 2)
    along = lax.rem(me + 2, 4)
    corner = lax.rem(across + 2, 4)
    return me, across, along, corner


def greet(axis, others):
    barrier = pltpu.get_barrier_semaphore()
    for other in others:
        pl.semaphore_signal(barrier, inc=1, device_id={axis: other}, device_id_type=MESH)
    pl.semaphore_wait(barrier, len(others))


def remote(axis, to, src, dst, send, recv):
    return pltpu.make_async_remote_copy(
        src_ref=src, dst_ref=dst, send_sem=send, recv_sem=recv, device_id={axis: to}, device_id_type=MESH
    )


def silu(v):
    return v / (1.0 + jnp.exp(-v))


def project_kernel(
    tok, w_x, w_z, w_bc, w_dt, bias, inner, gating, mapped, step,
    got, vx, vz, acc_x, acc_z, acc_m, acc_s, load, send, recv,
):
    me, across, along, corner = peers()
    rows, depth = tok.shape
    half = rows // 2
    lo, hi = pl.ds(0, half), pl.ds(half, half)
    loads = []
    owners = (me, across, along, corner)
    for k, owner in enumerate(owners):
        span = pl.ds(pl.multiple_of(owner * depth, LANES), depth)
        loads.append((
            pltpu.make_async_copy(w_x.at[span], vx.at[k], load.at[2 * k]),
            pltpu.make_async_copy(w_z.at[span], vz.at[k], load.at[2 * k + 1]),
        ))
    for pair in loads:
        for copy in pair:
            copy.start()
    greet("head", (across, along))
    copies = [
        remote("head", across, tok.at[lo], got.at[0, lo], send.at[0], recv.at[0]),
        remote("head", along, tok.at[hi], got.at[1, hi], send.at[1], recv.at[1]),
        remote("head", across, tok.at[hi], got.at[0, hi], send.at[2], recv.at[2]),
        remote("head", along, tok.at[lo], got.at[1, lo], send.at[3], recv.at[3]),
        remote("head", along, got.at[0, lo], got.at[2, lo], send.at[4], recv.at[4]),
        remote("head", across, got.at[1, hi], got.at[2, hi], send.at[5], recv.at[5]),
    ]
    for copy in copies[:4]:
        copy.start()

    wide = 256
    tiles = vx.shape[2] // wide

    def accumulate(k, block):
        for copy in loads[k]:
            copy.wait()
        span = pl.ds(pl.multiple_of(owners[k] * depth, LANES), depth)
        last = k == 3

        def tile(i, _):
            cols = pl.ds(pl.multiple_of(i * wide, wide), wide)
            a = jnp.dot(block[...], vx[k, :, cols], preferred_element_type=F32)
            b = jnp.dot(block[...], vz[k, :, cols], preferred_element_type=F32)
            if k:
                a, b = a + acc_x[:, cols], b + acc_z[:, cols]
            if last:
                inner[:, cols] = silu(a).astype(BF16)
                gating[:, cols] = b.astype(BF16)
            else:
                acc_x[:, cols] = a
                acc_z[:, cols] = b
            return 0

        lax.fori_loop(0, tiles, tile, 0)
        m = jnp.dot(block[...], w_bc[span, :], preferred_element_type=F32)
        s = jnp.dot(block[...], w_dt[span, :], preferred_element_type=F32)
        if k:
            m, s = m + acc_m[...], s + acc_s[...]
        if last:
            mapped[...] = silu(m).astype(BF16)
            v = s + bias[...]
            step[...] = jnp.zeros_like(step)
            step[:, : v.shape[1]] = jnp.maximum(v, 0.0) + jnp.log1p(jnp.exp(-jnp.abs(v)))
        else:
            acc_m[...] = m
            acc_s[...] = s

    accumulate(0, tok)
    copies[0].wait_recv()
    copies[4].start()
    copies[1].wait_recv()
    copies[5].start()
    copies[2].wait_recv()
    accumulate(1, got.at[0])
    copies[3].wait_recv()
    accumulate(2, got.at[1])
    copies[4].wait_recv()
    copies[5].wait_recv()
    accumulate(3, got.at[2])
    for copy in copies:
        copy.wait_send()


def project(tokens, w_x, w_z, w_bc, w_dt, dt_bias):
    rows, depth = tokens.shape
    width, heads, both = w_x.shape[1], w_dt.shape[1], w_bc.shape[1]
    padded = -(-heads // LANES) * LANES
    sds = jax.ShapeDtypeStruct
    return pl.pallas_call(
        project_kernel,
        out_shape=(
            sds((rows, width), BF16), sds((rows, width), BF16),
            sds((rows, both), BF16), sds((rows, padded), F32),
        ),
        in_specs=[VMEM, ANY, ANY, VMEM, VMEM, VMEM],
        out_specs=(VMEM,) * 4,
        scratch_shapes=[
            pltpu.VMEM((3, rows, depth), BF16),
            pltpu.VMEM((4, depth, width), BF16),
            pltpu.VMEM((4, depth, width), BF16),
            pltpu.VMEM((rows, width), F32),
            pltpu.VMEM((rows, width), F32),
            pltpu.VMEM((rows, both), F32),
            pltpu.VMEM((rows, heads), F32),
            pltpu.SemaphoreType.DMA((8,)),
            pltpu.SemaphoreType.DMA((6,)),
            pltpu.SemaphoreType.DMA((6,)),
        ],
        compiler_params=pltpu.CompilerParams(
            collective_id=0, has_side_effects=True, vmem_limit_bytes=60 * 1024 * 1024
        ),
    )(tokens, w_x, w_z, w_bc, w_dt, dt_bias.reshape(1, heads))


def scan_kernel(
    chain, heads, inner, gating, mapped, step, resets, rate, skip, gain, out, squares,
    cum, cumt, stept, keep, enter, score, local, first, thr, arrived, leaving, y, send, recv,
):
    me = lax.axis_index("seq")
    rows, width = inner.shape
    blocks = rows // GROUP
    pairs = width // LANES
    per = LANES // HEADDIM
    chunk = leaving.shape[2]
    chunks = width // chunk
    upper, lower = lax.rem(me + 1, chain), lax.rem(me + chain - 1, chain)
    greet("seq", (upper, lower))

    ti = lax.broadcasted_iota(jnp.int32, (GROUP, GROUP), 0)
    si = lax.broadcasted_iota(jnp.int32, (GROUP, GROUP), 1)
    causal = ti >= si
    tri = jnp.where(causal, 1.0, 0.0).astype(F32)
    lane = lax.broadcasted_iota(jnp.int32, (GROUP, LANES), 1)

    def column(ref, b, h):
        return jnp.sum(jnp.where(lane == h, ref[b], 0.0), axis=1, keepdims=True)

    def spread(ref, b, j):
        return jnp.where(lane < HEADDIM, column(ref, b, per * j), column(ref, b, per * j + 1))

    for b in range(blocks):
        span = pl.ds(b * GROUP, GROUP)
        stp = step[span, :]
        decay = -stp * rate[...]
        total = jnp.dot(tri, decay, preferred_element_type=F32, precision=lax.Precision.HIGHEST)
        cum[b] = total
        cumt[b] = total.T
        stept[b] = stp.T
        starts = resets[:, b * GROUP : (b + 1) * GROUP].astype(F32)
        seg_c = jnp.sum(tri * starts, axis=1, keepdims=True)
        start_c = jnp.sum(jnp.where(ti == si, jnp.broadcast_to(starts, (GROUP, GROUP)), 0.0), axis=1, keepdims=True)
        seg_r = jnp.sum(jnp.where(ti <= si, jnp.broadcast_to(start_c, (GROUP, GROUP)), 0.0), axis=0, keepdims=True)
        seg_end = seg_c[GROUP - 1 :, :]
        last = total[GROUP - 1 :, :]
        keep[b] = jnp.where(seg_c == seg_end, jnp.exp(last - total), 0.0) * stp
        enter[b] = jnp.where(seg_c == 0.0, jnp.exp(total), 0.0)
        bm, cm = mapped[span, :NSTATE], mapped[span, NSTATE:]
        dots = lax.dot_general(cm, bm, (((1,), (1,)), ((), ())), preferred_element_type=F32)
        score[b] = jnp.where(causal & (seg_c == seg_r), dots, 0.0)

    turned = [mapped[b * GROUP : (b + 1) * GROUP, :NSTATE].astype(F32).T.astype(BF16) for b in range(blocks)]

    def states(j, _):
        cols = pl.ds(pl.multiple_of(j * LANES, LANES), LANES)
        state = None
        for b in range(blocks):
            span = pl.ds(b * GROUP, GROUP)
            scaled = (spread(keep, b, j) * inner[span, cols].astype(F32)).astype(BF16)
            new = jnp.dot(turned[b], scaled, preferred_element_type=F32)
            through = spread(enter, b, j)[GROUP - 1 :, :]
            thr[b, :, cols] = through
            first[b, :, cols] = jnp.zeros((NSTATE, LANES), F32) if state is None else state
            state = new if state is None else through * state + new
        local[:, cols] = state
        return 0

    lax.fori_loop(0, pairs, states, 0)

    def down(c):
        return remote("seq", upper, leaving.at[c], arrived.at[c], send.at[c], recv.at[c])

    def combine(c, seen):
        cols = pl.ds(pl.multiple_of(c * chunk, chunk), chunk)
        value = local[:, cols]
        if seen:
            factor = thr[0, :, cols]
            for b in range(1, blocks):
                factor = factor * thr[b, :, cols]
            value = value + factor * arrived[c].astype(F32)
        leaving[c] = value.astype(BF16)
        down(c).start()

    @pl.when(me == 0)
    def _():
        arrived[...] = jnp.zeros_like(arrived)

        def turn(c, _):
            combine(c, False)
            return 0

        lax.fori_loop(0, chunks, turn, 0)

    offset = jnp.minimum(3 * me - 2, pairs - chunks)

    def within(j, _):
        cols = pl.ds(pl.multiple_of(j * LANES, LANES), LANES)
        for b in range(blocks):
            span = pl.ds(b * GROUP, GROUP)
            x = inner[span, cols]
            parts = []
            for k in range(per):
                h = per * j + k
                gap = column(cum, b, h) - cumt[b, pl.ds(h, 1), :]
                mixing = (jnp.exp(jnp.minimum(gap, 0.0)) * score[b] * stept[b, pl.ds(h, 1), :]).astype(BF16)
                parts.append(jnp.dot(mixing, x, preferred_element_type=F32))
            value = jnp.where(lane < HEADDIM, parts[0], parts[1])
            d = jnp.where(lane < HEADDIM, skip[per * j], skip[per * j + 1])
            y[span, cols] = value + d * x.astype(F32)
        c = j - offset

        @pl.when((me > 0) & (c >= 0) & (c < chunks))
        def _():
            down(c).wait_recv()

            @pl.when(me < chain - 1)
            def _():
                combine(c, True)

        return 0

    lax.fori_loop(0, pairs, within, 0)

    def finish(j, sums):
        cols = pl.ds(pl.multiple_of(j * LANES, LANES), LANES)
        tiles = chunk // LANES
        incoming = arrived[j // tiles, :, pl.ds(pl.multiple_of(lax.rem(j, tiles) * LANES, LANES), LANES)].astype(F32)
        new = []
        for b in range(blocks):
            span = pl.ds(b * GROUP, GROUP)
            state = first[b, :, cols] + incoming
            carried = jnp.dot(mapped[span, NSTATE:], state.astype(BF16), preferred_element_type=F32)
            value = y[span, cols] + spread(enter, b, j) * carried
            gated = value * silu(gating[span, cols].astype(F32))
            out[span, cols] = (gated * gain[:, cols]).astype(BF16)
            new.append(sums[b] + gated * gated)
            incoming = thr[b, :, cols] * incoming
        return tuple(new)

    sums = lax.fori_loop(0, pairs, finish, tuple(jnp.zeros((GROUP, LANES), F32) for _ in range(blocks)))
    for b in range(blocks):
        squares[:, b * GROUP : (b + 1) * GROUP] = lax.dot_general(
            jnp.ones((8, LANES), F32), sums[b], (((1,), (1,)), ((), ())),
            preferred_element_type=F32, precision=lax.Precision.HIGHEST,
        )

    @pl.when(me < chain - 1)
    def _():
        for c in range(chunks):
            down(c).wait_send()


def scan(chain, heads, inner, gating, mapped, step, resets, decay_rate, d_skip, norm_gain):
    rows, width = inner.shape
    blocks, padded = rows // GROUP, step.shape[1]
    chunk = 2 * LANES
    chunks = width // chunk
    sds = jax.ShapeDtypeStruct
    rate = jnp.pad(decay_rate.reshape(1, heads), ((0, 0), (0, padded - heads)))
    return pl.pallas_call(
        functools.partial(scan_kernel, chain, heads),
        out_shape=(sds((rows, width), BF16), sds((8, rows), F32)),
        in_specs=[VMEM] * 6 + [SMEM, VMEM],
        out_specs=(VMEM, VMEM),
        scratch_shapes=[
            pltpu.VMEM((blocks, GROUP, padded), F32),
            pltpu.VMEM((blocks, padded, GROUP), F32),
            pltpu.VMEM((blocks, padded, GROUP), F32),
            pltpu.VMEM((blocks, GROUP, padded), F32),
            pltpu.VMEM((blocks, GROUP, padded), F32),
            pltpu.VMEM((blocks, GROUP, GROUP), F32),
            pltpu.VMEM((NSTATE, width), F32),
            pltpu.VMEM((blocks, NSTATE, width), F32),
            pltpu.VMEM((blocks, 1, width), F32),
            pltpu.VMEM((chunks, NSTATE, chunk), BF16),
            pltpu.VMEM((chunks, NSTATE, chunk), BF16),
            pltpu.VMEM((rows, width), F32),
            pltpu.SemaphoreType.DMA((chunks,)),
            pltpu.SemaphoreType.DMA((chunks,)),
        ],
        compiler_params=pltpu.CompilerParams(
            collective_id=1, has_side_effects=True, vmem_limit_bytes=60 * 1024 * 1024
        ),
    )(inner, gating, mapped, step, resets.reshape(1, rows), rate, d_skip, norm_gain.reshape(1, width))


def output_kernel(total, g, squares, w, out, vw, others, sent, got, load, send, recv, sq_send, sq_recv):
    me, across, along, corner = peers()
    rows = g.shape[0]
    half = rows // 2
    width = out.shape[1]
    lo, hi = pl.ds(0, half), pl.ds(half, half)
    order = (corner, across, along, me)
    loads = [
        pltpu.make_async_copy(
            w.at[:, pl.ds(pl.multiple_of(owner * width, LANES), width)], vw.at[k], load.at[k]
        )
        for k, owner in enumerate(order)
    ]
    for copy in loads:
        copy.start()
    greet("head", (across, along, corner))
    small = [
        remote("head", to, squares, others.at[k], sq_send.at[k], sq_recv.at[k])
        for k, to in enumerate((across, along, corner))
    ]
    for copy in small:
        copy.start()

    def share(k, span):
        return jnp.dot(g[span, :], vw[k], preferred_element_type=F32)

    copies = [
        remote("head", to, sent.at[k], got.at[k], send.at[k], recv.at[k])
        for k, to in enumerate((across, along, across, along, along, across))
    ]

    def put(k, value):
        sent[k] = value.astype(BF16)
        copies[k].start()

    loads[0].wait()
    put(0, share(0, lo))
    put(1, share(0, hi))
    loads[1].wait()
    put(2, share(1, lo))
    loads[2].wait()
    put(3, share(2, hi))
    value = share(2, lo)
    copies[0].wait_recv()
    put(4, value + got[0].astype(F32))
    value = share(1, hi)
    copies[1].wait_recv()
    put(5, value + got[1].astype(F32))
    loads[3].wait()
    for copy in small:
        copy.wait_recv()
    squared = squares[...] + others[0] + others[1] + others[2]
    scale = lax.rsqrt(squared / total + EPS)
    scale = jnp.broadcast_to(scale[:1, :], (LANES, rows)).T
    for span, base, pick in ((lo, 0, (2, 4)), (hi, half, (3, 5))):
        value = share(3, span)
        for k in pick:
            copies[k].wait_recv()
            value = value + got[k].astype(F32)
        factor = scale[base : base + half, :]
        for i in range(width // LANES):
            cols = slice(i * LANES, (i + 1) * LANES)
            out[span, cols] = (value[:, cols] * factor).astype(BF16)
    for copy in copies + small:
        copy.wait_send()


def output(total, g, squares, w_out, width):
    rows, depth = g.shape
    half = rows // 2
    return pl.pallas_call(
        functools.partial(output_kernel, total),
        out_shape=jax.ShapeDtypeStruct((rows, width), BF16),
        in_specs=[VMEM, VMEM, ANY],
        out_specs=VMEM,
        scratch_shapes=[
            pltpu.VMEM((4, depth, width), BF16),
            pltpu.VMEM((3, 8, rows), F32),
            pltpu.VMEM((6, half, width), BF16),
            pltpu.VMEM((6, half, width), BF16),
            pltpu.SemaphoreType.DMA((4,)),
            pltpu.SemaphoreType.DMA((6,)),
            pltpu.SemaphoreType.DMA((6,)),
            pltpu.SemaphoreType.DMA((3,)),
            pltpu.SemaphoreType.DMA((3,)),
        ],
        compiler_params=pltpu.CompilerParams(
            collective_id=2, has_side_effects=True, vmem_limit_bytes=60 * 1024 * 1024
        ),
    )(g, squares, w_out)


def solution(mesh):
    chain, split = mesh.shape["seq"], mesh.shape["head"]

    def on_device(tokens, resets, w_x, w_z, w_bc, w_dt, dt_bias, decay_rate, d_skip, norm_gain, w_out):
        inner, gating, mapped, step = project(tokens, w_x, w_z, w_bc, w_dt, dt_bias)
        g, squares = scan(
            chain, w_dt.shape[1], inner, gating, mapped, step, resets, decay_rate, d_skip, norm_gain
        )
        return output(float(w_x.shape[1] * split), g, squares, w_out, tokens.shape[1])

    in_specs = (
        P(("batch", "seq"), "head"),
        P(("batch", "seq")),
        P(None, "head"),
        P(None, "head"),
        P(),
        P(None, "head"),
        P("head"),
        P("head"),
        P("head"),
        P("head"),
        P("head", None),
    )
    return jax.shard_map(
        on_device, mesh=mesh, in_specs=in_specs, out_specs=P(("batch", "seq"), "head"), check_vma=False
    )
```

```python
import functools

import jax
import jax.numpy as jnp
from jax import lax
from jax.experimental import pallas as pl
from jax.experimental.pallas import tpu as pltpu
from jax.sharding import PartitionSpec as P

HEADDIM = 64
NSTATE = 128
GROUP = 256
LANES = 128
F32 = jnp.float32
BF16 = jnp.bfloat16
MESH = pl.DeviceIdType.MESH
VMEM = pl.BlockSpec(memory_space=pltpu.VMEM)
SMEM = pl.BlockSpec(memory_space=pltpu.SMEM)
ANY = pl.BlockSpec(memory_space=pl.ANY)
EPS = 1e-05


def peers():
    me = lax.axis_index("head")
    across = me + 1 - 2 * lax.rem(me, 2)
    along = lax.rem(me + 2, 4)
    corner = lax.rem(across + 2, 4)
    return me, across, along, corner


def remote(axis, to, src, dst, send, recv):
    return pltpu.make_async_remote_copy(
        src_ref=src, dst_ref=dst, send_sem=send, recv_sem=recv, device_id={axis: to}, device_id_type=MESH
    )


def silu(v):
    return v / (1.0 + jnp.exp(-v))


class Scratch:
    def __init__(self, names, refs):
        for name, ref in zip(names, refs):
            setattr(self, name, ref)


def dot(a, b):
    return jnp.dot(a, b, preferred_element_type=F32)


def dot_nt(a, b, precision=None):
    return lax.dot_general(a, b, (((1,), (1,)), ((), ())), preferred_element_type=F32, precision=precision)


def kernel(chain, total, names, tok, resets, w_x, w_z, w_bc, w_dt, bias, rate, skip, gain, w_out, out, *refs):
    r = Scratch(names, refs)
    me, across, along, corner = peers()
    pos = lax.axis_index("seq")
    upper, lower = lax.rem(pos + 1, chain), lax.rem(pos + chain - 1, chain)
    rows, depth = tok.shape
    width = w_x.shape[1]
    heads = w_dt.shape[0]
    blocks, pairs, per = rows // GROUP, width // LANES, LANES // HEADDIM
    half = GROUP // 2
    owners = (me, across, along, corner)

    def span_of(owner):
        return pl.ds(pl.multiple_of(owner * depth, LANES), depth)

    def rows_of(b):
        return pl.ds(b * GROUP, GROUP)

    def cols_of(j):
        return pl.ds(pl.multiple_of(j * LANES, LANES), LANES)

    loads = [
        (
            pltpu.make_async_copy(w_x.at[span_of(owner)], r.vx.at[k], r.load.at[3 * k]),
            pltpu.make_async_copy(w_z.at[span_of(owner)], r.vz.at[k], r.load.at[3 * k + 1]),
            pltpu.make_async_copy(w_bc.at[span_of(owner)], r.vb.at[k], r.load.at[3 * k + 2]),
        )
        for k, owner in enumerate(owners)
    ]
    order = (corner, across, along, me)
    out_loads = [
        pltpu.make_async_copy(w_out.at[:, span_of(owner)], r.vw.at[k], r.load_out.at[k])
        for k, owner in enumerate(order)
    ]
    for k in (0, 1):
        for copy in loads[k]:
            copy.start()

    barrier = pltpu.get_barrier_semaphore()
    for other in (across, along, corner):
        pl.semaphore_signal(barrier, inc=1, device_id={"head": other}, device_id_type=MESH)
    for other in (upper, lower):
        pl.semaphore_signal(barrier, inc=1, device_id={"seq": other}, device_id_type=MESH)
    pl.semaphore_wait(barrier, 5)

    gathers = []
    for b in range(blocks):
        lo, hi = pl.ds(b * GROUP, half), pl.ds(b * GROUP + half, half)
        plan = (
            (across, tok.at[lo], r.got.at[0, lo]),
            (along, tok.at[hi], r.got.at[1, hi]),
            (across, tok.at[hi], r.got.at[0, hi]),
            (along, tok.at[lo], r.got.at[1, lo]),
            (along, r.got.at[0, lo], r.got.at[2, lo]),
            (across, r.got.at[1, hi], r.got.at[2, hi]),
        )
        gathers.append([
            remote("head", to, src, dst, r.g_send.at[6 * b + i], r.g_recv.at[6 * b + i])
            for i, (to, src, dst) in enumerate(plan)
        ])
    for copy in gathers[0][:4]:
        copy.start()

    wide = 256

    def accumulate(b, k):
        if b == 0:
            for copy in loads[k]:
                copy.wait()
            if k == 0:
                for later in (2, 3):
                    for copy in loads[later]:
                        copy.start()
            if k == 3:
                for copy in out_loads:
                    copy.start()
        rs = rows_of(b)
        block = tok if k == 0 else r.got.at[k - 1]

        def tile(i, _):
            cols = pl.ds(pl.multiple_of(i * wide, wide), wide)
            x = block[rs, :]
            v, z = dot(x, r.vx[k, :, cols]), dot(x, r.vz[k, :, cols])
            if k:
                v, z = v + r.acc_x[:, cols], z + r.acc_z[:, cols]
            if k == 3:
                r.inner[rs, cols] = silu(v).astype(BF16)
                r.gating[rs, cols] = z.astype(BF16)
            else:
                r.acc_x[:, cols] = v
                r.acc_z[:, cols] = z
            return 0

        lax.fori_loop(0, width // wide, tile, 0)
        m = dot(block[rs, :], r.vb[k])
        s = dot_nt(block[rs, :], w_dt[:, span_of(owners[k])])
        if k:
            m, s = m + r.acc_m[...], s + r.acc_s[...]
        if k == 3:
            r.mapped[rs, :] = silu(m).astype(BF16)
            v = s + bias[...]
            r.step[...] = jnp.zeros_like(r.step)
            r.step[:, :heads] = jnp.maximum(v, 0.0) + jnp.log1p(jnp.exp(-jnp.abs(v)))
        else:
            r.acc_m[...] = m
            r.acc_s[...] = s

    def relay(b):
        gathers[b][0].wait_recv()
        gathers[b][4].start()
        gathers[b][1].wait_recv()
        gathers[b][5].start()
        if b + 1 < blocks:
            for copy in gathers[b + 1][:4]:
                copy.start()

    def project(b):
        gathers[b][2].wait_recv()
        accumulate(b, 1)
        gathers[b][3].wait_recv()
        accumulate(b, 2)
        gathers[b][4].wait_recv()
        gathers[b][5].wait_recv()
        accumulate(b, 3)

    ti = lax.broadcasted_iota(jnp.int32, (GROUP, GROUP), 0)
    si = lax.broadcasted_iota(jnp.int32, (GROUP, GROUP), 1)
    causal = ti >= si
    tri = jnp.where(causal, 1.0, 0.0).astype(F32)
    lane = lax.broadcasted_iota(jnp.int32, (GROUP, LANES), 1)
    r.rate[...] = jnp.zeros_like(r.rate)
    r.rate[:, :heads] = rate[...]

    def column(ref, b, h):
        return jnp.sum(jnp.where(lane == h, ref[b], 0.0), axis=1, keepdims=True)

    def spread(ref, b, j):
        return jnp.where(lane < HEADDIM, column(ref, b, per * j), column(ref, b, per * j + 1))

    def prepare(b):
        rs = rows_of(b)
        stp = r.step[...]
        decay = -stp * r.rate[...]
        cum = jnp.dot(tri, decay, preferred_element_type=F32, precision=lax.Precision.HIGHEST)
        r.cum[b] = cum
        r.cumt[b] = cum.T
        r.stept[b] = stp.T
        starts = resets[:, b * GROUP : (b + 1) * GROUP].astype(F32)
        whole = jnp.broadcast_to(starts, (GROUP, GROUP))
        seg_c = jnp.sum(tri * starts, axis=1, keepdims=True)
        start_c = jnp.sum(jnp.where(ti == si, whole, 0.0), axis=1, keepdims=True)
        seg_r = jnp.sum(jnp.where(ti <= si, jnp.broadcast_to(start_c, (GROUP, GROUP)), 0.0), axis=0, keepdims=True)
        last = cum[GROUP - 1 :, :]
        r.keep[b] = jnp.where(seg_c == seg_c[GROUP - 1 :, :], jnp.exp(last - cum), 0.0) * stp
        r.enter[b] = jnp.where(seg_c == 0.0, jnp.exp(cum), 0.0)
        dots = dot_nt(r.mapped[rs, NSTATE:], r.mapped[rs, :NSTATE])
        r.score[b] = jnp.where(causal & (seg_c == seg_r), dots, 0.0)

    def states(b):
        rs = rows_of(b)
        turned = r.mapped[rs, :NSTATE].astype(F32).T.astype(BF16)

        def turn(j, _):
            cols = cols_of(j)
            scaled = (spread(r.keep, b, j) * r.inner[rs, cols].astype(F32)).astype(BF16)
            new = dot(turned, scaled)
            through = spread(r.enter, b, j)[GROUP - 1 :, :]
            r.thr[b, :, cols] = through
            if b:
                new = new + through * r.state[b - 1, :, cols]
            r.state[b, :, cols] = new
            if b == blocks - 1:

                @pl.when(pos == 0)
                def _():
                    combine(j, False)

            return 0

        lax.fori_loop(0, pairs, turn, 0)

    def down(c):
        return remote("seq", upper, r.leaving.at[c], r.arrived.at[c], r.c_send.at[c], r.c_recv.at[c])

    def combine(c, seen):
        cols = cols_of(c)
        value = r.state[blocks - 1, :, cols]
        if seen:
            factor = r.thr[0, :, cols]
            for b in range(1, blocks):
                factor = factor * r.thr[b, :, cols]
            value = value + factor * r.arrived[c].astype(F32)
        r.leaving[c] = value.astype(BF16)
        down(c).start()

    def receive(c):
        down(c).wait_recv()

        @pl.when(pos < chain - 1)
        def _():
            combine(c, True)

    early = pairs // 2

    def within(b):
        rs = rows_of(b)

        def turn(j, _):
            cols = cols_of(j)
            x = r.inner[rs, cols]
            parts = []
            for k in range(per):
                h = per * j + k
                gap = column(r.cum, b, h) - r.cumt[b, pl.ds(h, 1), :]
                weight = jnp.exp(jnp.minimum(gap, 0.0)) * r.score[b] * r.stept[b, pl.ds(h, 1), :]
                parts.append(dot(weight.astype(BF16), x))
            d = jnp.where(lane < HEADDIM, skip[per * j], skip[per * j + 1])
            r.y[rs, cols] = jnp.where(lane < HEADDIM, parts[0], parts[1]) + d * x.astype(F32)
            if b == blocks - 1:

                @pl.when((pos == 1) & (j >= early))
                def _():
                    receive(j - early)

            return 0

        lax.fori_loop(0, pairs, turn, 0)

    @pl.when(pos == 0)
    def _():
        r.arrived[...] = jnp.zeros_like(r.arrived)

    accumulate(0, 0)
    relay(0)
    project(0)
    prepare(0)
    states(0)
    for b in range(1, blocks):
        relay(b)
        within(b - 1)
        accumulate(b, 0)
        project(b)
        prepare(b)
        states(b)
    within(blocks - 1)

    r.sums[...] = jnp.zeros_like(r.sums)

    def finish(j, _):
        @pl.when((pos > 1) | ((pos == 1) & (j >= pairs - early)))
        def _():
            receive(j)

        cols = cols_of(j)
        incoming = r.arrived[j].astype(F32)
        for b in range(blocks):
            rs = rows_of(b)
            state = incoming + r.state[b - 1, :, cols] if b else incoming
            carried = dot(r.mapped[rs, NSTATE:], state.astype(BF16))
            value = r.y[rs, cols] + spread(r.enter, b, j) * carried
            gated = value * silu(r.gating[rs, cols].astype(F32))
            r.g[rs, cols] = (gated * gain[pl.ds(j, 1), :]).astype(BF16)
            r.sums[rs, :] = r.sums[rs, :] + gated * gated
            incoming = r.thr[b, :, cols] * incoming
        return 0

    lax.fori_loop(0, pairs, finish, 0)

    for copy in out_loads:
        copy.wait()
    small = [
        remote("head", to, r.squares, r.others.at[k], r.q_send.at[k], r.q_recv.at[k])
        for k, to in enumerate((across, along, corner))
    ]
    scatters = [
        [
            remote("head", to, r.sent.at[6 * b + k], r.back.at[6 * b + k], r.o_send.at[6 * b + k], r.o_recv.at[6 * b + k])
            for k, to in enumerate((across, along, across, along, along, across))
        ]
        for b in range(blocks)
    ]

    def put(b, k, value):
        r.sent[6 * b + k] = value.astype(BF16)
        scatters[b][k].start()

    def share(k, rs):
        return dot(r.g[rs, :], r.vw[k])

    def direct(b):
        lo, hi = pl.ds(b * GROUP, half), pl.ds(b * GROUP + half, half)
        put(b, 0, share(0, lo))
        put(b, 1, share(0, hi))
        put(b, 2, share(1, lo))
        put(b, 3, share(2, hi))

    def joined(b):
        lo, hi = pl.ds(b * GROUP, half), pl.ds(b * GROUP + half, half)
        value = share(2, lo)
        scatters[b][0].wait_recv()
        put(b, 4, value + r.back[6 * b].astype(F32))
        value = share(1, hi)
        scatters[b][1].wait_recv()
        put(b, 5, value + r.back[6 * b + 1].astype(F32))

    for b in range(blocks):
        direct(b)
        if b == 0:
            r.squares[...] = dot_nt(jnp.ones((8, LANES), F32), r.sums[...], lax.Precision.HIGHEST)
            for copy in small:
                copy.start()
        if b:
            joined(b - 1)
    joined(blocks - 1)
    own = r.y
    for b in range(blocks):
        own[rows_of(b), :depth] = share(3, rows_of(b))
    for copy in small:
        copy.wait_recv()
    squared = r.squares[...] + r.others[0] + r.others[1] + r.others[2]
    scale = lax.rsqrt(squared / total + EPS)
    r.sums[...] = jnp.broadcast_to(scale[:1, :], (LANES, rows)).T
    for b in range(blocks):
        for base, picks in ((b * GROUP, (2, 4)), (b * GROUP + half, (3, 5))):
            span = pl.ds(base, half)
            for k in picks:
                scatters[b][k].wait_recv()
            for i in range(depth // LANES):
                cols = slice(i * LANES, (i + 1) * LANES)
                value = own[span, cols]
                for k in picks:
                    value = value + r.back[6 * b + k, :, cols].astype(F32)
                out[span, cols] = (value * r.sums[span, :]).astype(BF16)

    for group in gathers + scatters + [small]:
        for copy in group:
            copy.wait_send()

    @pl.when(pos < chain - 1)
    def _():
        for c in range(pairs):
            down(c).wait_send()


def layer(chain, split, tokens, resets, w_x, w_z, w_bc, w_dt, dt_bias, decay_rate, d_skip, norm_gain, w_out):
    rows, depth = tokens.shape
    width, heads, both = w_x.shape[1], w_dt.shape[1], w_bc.shape[1]
    padded = -(-heads // LANES) * LANES
    blocks, pairs = rows // GROUP, width // LANES
    half = GROUP // 2
    vm, dma = pltpu.VMEM, pltpu.SemaphoreType.DMA
    scratch = dict(
        got=vm((3, rows, depth), BF16),
        vx=vm((4, depth, width), BF16),
        vz=vm((4, depth, width), BF16),
        vb=vm((4, depth, both), BF16),
        vw=vm((4, width, depth), BF16),
        acc_x=vm((GROUP, width), F32),
        acc_z=vm((GROUP, width), F32),
        acc_m=vm((GROUP, both), F32),
        acc_s=vm((GROUP, heads), F32),
        inner=vm((rows, width), BF16),
        gating=vm((rows, width), BF16),
        mapped=vm((rows, both), BF16),
        step=vm((GROUP, padded), F32),
        rate=vm((1, padded), F32),
        cum=vm((blocks, GROUP, padded), F32),
        cumt=vm((blocks, padded, GROUP), F32),
        stept=vm((blocks, padded, GROUP), F32),
        keep=vm((blocks, GROUP, padded), F32),
        enter=vm((blocks, GROUP, padded), F32),
        score=vm((blocks, GROUP, GROUP), F32),
        state=vm((blocks, NSTATE, width), F32),
        thr=vm((blocks, 1, width), F32),
        arrived=vm((pairs, NSTATE, LANES), BF16),
        leaving=vm((pairs, NSTATE, LANES), BF16),
        y=vm((rows, width), F32),
        g=vm((rows, width), BF16),
        sums=vm((rows, LANES), F32),
        squares=vm((8, rows), F32),
        others=vm((3, 8, rows), F32),
        sent=vm((6 * blocks, half, depth), BF16),
        back=vm((6 * blocks, half, depth), BF16),
        load=dma((12,)),
        load_out=dma((4,)),
        g_send=dma((6 * blocks,)),
        g_recv=dma((6 * blocks,)),
        c_send=dma((pairs,)),
        c_recv=dma((pairs,)),
        o_send=dma((6 * blocks,)),
        o_recv=dma((6 * blocks,)),
        q_send=dma((3,)),
        q_recv=dma((3,)),
    )
    return pl.pallas_call(
        functools.partial(kernel, chain, float(width * split), tuple(scratch)),
        out_shape=jax.ShapeDtypeStruct((rows, depth), BF16),
        in_specs=[VMEM, VMEM, ANY, ANY, ANY, VMEM, VMEM, VMEM, SMEM, VMEM, ANY],
        out_specs=VMEM,
        scratch_shapes=list(scratch.values()),
        compiler_params=pltpu.CompilerParams(
            collective_id=0, has_side_effects=True, vmem_limit_bytes=60 * 1024 * 1024
        ),
    )(
        tokens, resets.reshape(1, rows), w_x, w_z, w_bc, w_dt.T, dt_bias.reshape(1, heads),
        decay_rate.reshape(1, heads), d_skip, norm_gain.reshape(pairs, LANES), w_out,
    )


def solution(mesh):
    in_specs = (
        P(("batch", "seq"), "head"),
        P(("batch", "seq")),
        P(None, "head"),
        P(None, "head"),
        P(),
        P(None, "head"),
        P("head"),
        P("head"),
        P("head"),
        P("head"),
        P("head", None),
    )
    return jax.shard_map(
        functools.partial(layer, mesh.shape["seq"], mesh.shape["head"]),
        mesh=mesh,
        in_specs=in_specs,
        out_specs=P(("batch", "seq"), "head"),
        check_vma=False,
    )
```
